32 devices in a mesh: wall: 4 (over z), span: 8 (over y, x, core).
Axes of the slice: x: 2, y: 2, z: 4, core: 2. Of those that a mesh axis runs over, the one named last changes fastest.
Arguments:
- noise_bits: int32 [3, 32, 512, 1024], P(None, None, 'span', 'wall'), may hold values from 0 to 1073741823
- filter_widths: int32 [1024], P('wall'), may hold values from 8 to 64, as said below
- target_mean_profile: float32 [3, 1024], P(None, 'wall'), may hold values from -4 to 4
- target_factor_diagonal: float32 [3, 1024], P(None, 'wall'), may hold values from 0.3 to 2
- target_factor_lower: float32 [3, 1024], P(None, 'wall'), may hold values from -0.8 to 0.8
Outputs:
- inflow_field: float32 [3, 32, 512, 1024], P(None, None, 'span', 'wall')
The draws below stay inside these ranges and needn't reach their ends.
Inputs may be any that keep to these rules, and one draw needn't show every extreme that they name: `filter_widths`: every row's width lies between 8 and 64, and both ends occur in every draw.
All inputs are finite; a program needn't handle non-finite values.
Results may differ from the reference program's by a relative error of at most 0.0045.
Values may be sent and summed in bfloat16 or wider, within the bound.
A program may use at most 64 MiB of HBM per device.

```python
import math
import jax
import jax.numpy as jnp
from jax import lax

NC = 3
SAMPLES = 32
ROWS_PER_UNIT = 256
COLS_DEV = 64
WMAX = 64
SPANW = 32
TSCALE = 8
NY = 1024
NZ = 512
N_WALL = 4


def draw_filter_widths(key, part):
    lowest = WMAX // 8
    sampled = jax.random.randint(key, (NY,), lowest, WMAX + 1)
    chosen = jax.random.randint(jax.random.fold_in(key, 7), (), 0, NY)
    sampled = sampled.at[chosen].set(WMAX)
    partner = (chosen + NY // 2) % NY
    return sampled.at[partner].set(lowest).astype(jnp.int32)


def place_ends(drawn, own_key, low, top_value):
    place = [jax.random.randint(jax.random.fold_in(own_key, axis), (), 0, length) for axis, length in enumerate(drawn.shape)]
    longest = drawn.shape.index(max(drawn.shape))
    beside = place[:longest] + [(place[longest] + 1) % drawn.shape[longest]] + place[longest + 1:]
    return drawn.at[tuple(place)].set(low).at[tuple(beside)].set(top_value)


def levels(own_key, shape, split, least, high):
    def one(position, blocks):
        steps = jax.random.uniform(jax.random.fold_in(jax.random.fold_in(own_key, 6), position), (blocks,), jnp.float32, least / len(split), high / len(split))
        return jnp.repeat(jnp.exp(steps), shape[position] // blocks).reshape((-1,) + (1,) * (len(shape) - position - 1))

    loudness = one(*split[0])
    for cut in split[1:]:
        loudness = loudness * one(*cut)
    return loudness


def gaussian(key, extent, scale, most, cuts=(), dtype=jnp.bfloat16):
    entries = scale * jax.random.normal(key, extent, jnp.float32)
    if cuts:
        entries = entries * levels(key, extent, cuts, -0.22, 0.18)
    return jnp.clip(entries, -most, most).astype(dtype)


def setup_inputs(seed: int = 0) -> dict:
    keys = jax.random.split(jax.random.key(seed), 6)
    return {
        "noise_bits": place_ends(jax.random.randint(keys[0], (NC, SAMPLES, NZ, NY), 0, 1073741824), jax.random.fold_in(keys[0], 1), 0, 1073741823).astype(jnp.int32),
        "filter_widths": draw_filter_widths(jax.random.fold_in(keys[5], 71), 0),
        "target_mean_profile": gaussian(keys[2], (NC, NY), 1.0, 4.0, ((1, 4),), jnp.float32),
        "target_factor_diagonal": jnp.clip(jnp.exp(math.log(2.0) - 1.89712 * jax.random.uniform(keys[3], (NC, NY), jnp.float32) ** levels(keys[3], (NC, NY), ((1, 4),), -0.2, 0.2)), 0.3, 2.0),
        "target_factor_lower": jnp.clip(jax.random.uniform(keys[4], (NC, NY), jnp.float32, -0.8, 0.8) * levels(keys[4], (NC, NY), ((1, 4),), -0.4, 0.0), -0.8, 0.8),
    }


PAIRS = ((0, 0), (1, 0), (1, 1), (2, 0), (2, 1), (2, 2))
SPREAD_FLOOR = 0.25
INV_RANGE = 1.0 / 1073741824.0

def to_field(noise_bits):
    scaled = (noise_bits.astype(jnp.float32) + 0.5) * INV_RANGE - 0.5
    return (math.sqrt(12.0) * scaled).astype(jnp.bfloat16)

def band_matrix(cell_widths, in_count, margin):
    out_count = cell_widths.shape[0]
    offsets = (lax.broadcasted_iota(jnp.int32, (out_count, in_count), 1) - margin - lax.broadcasted_iota(jnp.int32, (out_count, in_count), 0)).astype(jnp.float32)
    spread = cell_widths[:, None]
    inside = jnp.abs(offsets) <= 2.0 * spread
    safe_off = jnp.where(inside, offsets, 0.0)
    kernel = jnp.where(inside, jnp.exp(-math.pi * safe_off * safe_off / (8.0 * spread * spread)), 0.0)
    norm_total = jnp.sqrt(lax.optimization_barrier(jnp.sum(kernel * kernel, axis=1, keepdims=True)))
    return (kernel / norm_total).astype(jnp.bfloat16)

def time_matrix(sample_count):
    later_idx = lax.broadcasted_iota(jnp.int32, (sample_count, sample_count), 0)
    earlier = lax.broadcasted_iota(jnp.int32, (sample_count, sample_count), 1)
    causal = later_idx >= earlier
    lagged = jnp.where(causal, later_idx - earlier, 0).astype(jnp.float32)
    decay_rate = math.exp(-math.pi / (2.0 * TSCALE))
    fresh_gain = jnp.where(earlier == 0, 1.0, math.sqrt(1.0 - decay_rate * decay_rate))
    return jnp.where(causal, jnp.exp(-math.pi * lagged / (2.0 * TSCALE)) * fresh_gain, 0.0).astype(jnp.float32)

def lund_transform(sample_covariance, target_factor_diagonal, target_factor_lower):
    cov_00 = sample_covariance[0] + SPREAD_FLOOR
    cov_10 = sample_covariance[1]
    cov_11 = sample_covariance[2] + SPREAD_FLOOR
    cov_20 = sample_covariance[3]
    cov_21 = sample_covariance[4]
    cov_22 = sample_covariance[5] + SPREAD_FLOOR
    chol_00 = jnp.sqrt(cov_00)
    chol_10 = cov_10 / chol_00
    chol_20 = cov_20 / chol_00
    chol_11 = jnp.sqrt(cov_11 - chol_10 * chol_10)
    chol_21 = (cov_21 - chol_20 * chol_10) / chol_11
    chol_22 = jnp.sqrt(cov_22 - chol_20 * chol_20 - chol_21 * chol_21)
    inv_00 = 1.0 / chol_00
    inv_11 = 1.0 / chol_11
    inv_22 = 1.0 / chol_22
    inv_10 = -chol_10 * inv_00 * inv_11
    inv_21 = -chol_21 * inv_11 * inv_22
    inv_20 = -(chol_20 * inv_00 + chol_21 * inv_10) * inv_22
    gain_00 = target_factor_diagonal[0] * inv_00
    gain_10 = target_factor_lower[0] * inv_00 + target_factor_diagonal[1] * inv_10
    gain_11 = target_factor_diagonal[1] * inv_11
    gain_20 = target_factor_lower[1] * inv_00 + target_factor_lower[2] * inv_10 + target_factor_diagonal[2] * inv_20
    gain_21 = target_factor_lower[2] * inv_11 + target_factor_diagonal[2] * inv_21
    gain_22 = target_factor_diagonal[2] * inv_22
    return jnp.stack([gain_00, gain_10, gain_11, gain_20, gain_21, gain_22])

def rescaled_inflow(fluctuation, per_row_means, scaling_terms, velocity_profile):
    centred_samples = fluctuation - per_row_means[:, None, None, :]
    first_component = velocity_profile[0] + scaling_terms[0] * centred_samples[0]
    second_component = velocity_profile[1] + scaling_terms[1] * centred_samples[0] + scaling_terms[2] * centred_samples[1]
    third_component = velocity_profile[2] + scaling_terms[3] * centred_samples[0] + scaling_terms[4] * centred_samples[1] + scaling_terms[5] * centred_samples[2]
    return jnp.stack([first_component, second_component, third_component])

def reference(noise_bits, filter_widths, target_mean_profile, target_factor_diagonal, target_factor_lower):
    margin = 2 * WMAX
    span_margin = 2 * SPANW
    psi_field = to_field(noise_bits)
    padded = jnp.pad(psi_field, ((0, 0), (0, 0), (0, 0), (margin, margin)))
    span_band = band_matrix(jnp.full((COLS_DEV,), float(SPANW), jnp.float32), COLS_DEV + 2 * span_margin, span_margin).astype(jnp.float32)
    memory = time_matrix(SAMPLES)
    cell_count = float(SAMPLES * NZ)

    def one_block(block_idx, output):
        first_row_index = (block_idx * ROWS_PER_UNIT).astype(jnp.int32)
        window = lax.dynamic_slice_in_dim(padded, first_row_index, ROWS_PER_UNIT + 2 * margin, 3)
        row_widths = lax.dynamic_slice_in_dim(filter_widths, first_row_index, ROWS_PER_UNIT, 0)
        wall_band = band_matrix(row_widths.astype(jnp.float32), ROWS_PER_UNIT + 2 * margin, margin)
        smooth = jnp.einsum('csjm,ym->csjy', window.astype(jnp.float32), wall_band.astype(jnp.float32)).astype(jnp.bfloat16)
        blocks = smooth.reshape(NC, SAMPLES, NZ // COLS_DEV, COLS_DEV, ROWS_PER_UNIT)
        left_edge = jnp.roll(blocks, 1, axis=2)[:, :, :, COLS_DEV - span_margin:]
        right_edge = jnp.roll(blocks, -1, axis=2)[:, :, :, :span_margin]
        widened = jnp.concatenate([left_edge, blocks, right_edge], axis=3).astype(jnp.float32)
        spanned = jnp.einsum('kj,csbjy->csbky', span_band, widened).reshape(NC, SAMPLES, NZ, ROWS_PER_UNIT)
        fluctuation = jnp.einsum('ts,csky->ctky', memory, spanned, precision=lax.Precision.HIGHEST)
        per_row_means = lax.optimization_barrier(jnp.sum(fluctuation, axis=(1, 2))) / cell_count
        centred_samples = fluctuation - per_row_means[:, None, None, :]
        sample_covariance = jnp.stack([lax.optimization_barrier(jnp.sum(centred_samples[first_c] * centred_samples[second_c], axis=(0, 1))) for first_c, second_c in PAIRS]) / cell_count
        scaling_terms = lund_transform(sample_covariance, lax.dynamic_slice_in_dim(target_factor_diagonal, first_row_index, ROWS_PER_UNIT, 1), lax.dynamic_slice_in_dim(target_factor_lower, first_row_index, ROWS_PER_UNIT, 1))
        final_result = rescaled_inflow(fluctuation, per_row_means, scaling_terms, lax.dynamic_slice_in_dim(target_mean_profile, first_row_index, ROWS_PER_UNIT, 1))
        return lax.dynamic_update_slice_in_dim(output, final_result, first_row_index, 3)
    output = jnp.zeros((NC, SAMPLES, NZ, NY), jnp.float32)
    return lax.fori_loop(0, N_WALL, one_block, output)
```

```python
import functools
import math

import jax
import jax.numpy as jnp
from jax import lax
from jax.experimental import pallas as pl
from jax.experimental.pallas import tpu as pltpu
from jax.sharding import PartitionSpec as P

WMAX = 64
SPANW = 32
TSCALE = 8


PAIRS = ((0, 0), (1, 0), (1, 1), (2, 0), (2, 1), (2, 2))
SPREAD_FLOOR = 0.25
INV_RANGE = 1.0 / 1073741824.0


def to_field(noise_bits):
    scaled = (noise_bits.astype(jnp.float32) + 0.5) * INV_RANGE - 0.5
    return (math.sqrt(12.0) * scaled).astype(jnp.bfloat16)


def lund_transform(sample_covariance, target_factor_diagonal, target_factor_lower):
    cov_00 = sample_covariance[0] + SPREAD_FLOOR
    cov_10 = sample_covariance[1]
    cov_11 = sample_covariance[2] + SPREAD_FLOOR
    cov_20 = sample_covariance[3]
    cov_21 = sample_covariance[4]
    cov_22 = sample_covariance[5] + SPREAD_FLOOR
    chol_00 = jnp.sqrt(cov_00)
    chol_10 = cov_10 / chol_00
    chol_20 = cov_20 / chol_00
    chol_11 = jnp.sqrt(cov_11 - chol_10 * chol_10)
    chol_21 = (cov_21 - chol_20 * chol_10) / chol_11
    chol_22 = jnp.sqrt(cov_22 - chol_20 * chol_20 - chol_21 * chol_21)
    inv_00 = 1.0 / chol_00
    inv_11 = 1.0 / chol_11
    inv_22 = 1.0 / chol_22
    inv_10 = -chol_10 * inv_00 * inv_11
    inv_21 = -chol_21 * inv_11 * inv_22
    inv_20 = -(chol_20 * inv_00 + chol_21 * inv_10) * inv_22
    gain_00 = target_factor_diagonal[0] * inv_00
    gain_10 = target_factor_lower[0] * inv_00 + target_factor_diagonal[1] * inv_10
    gain_11 = target_factor_diagonal[1] * inv_11
    gain_20 = (
        target_factor_lower[1] * inv_00
        + target_factor_lower[2] * inv_10
        + target_factor_diagonal[2] * inv_20
    )
    gain_21 = target_factor_lower[2] * inv_11 + target_factor_diagonal[2] * inv_21
    gain_22 = target_factor_diagonal[2] * inv_22
    return gain_00, gain_10, gain_11, gain_20, gain_21, gain_22


CHUNK = 2
AHEAD = 4
BLOCK = 4
MESH = pl.DeviceIdType.MESH


def band_taps(offsets, spread, axis):
    inside = jnp.abs(offsets) <= 2.0 * spread
    safe_off = jnp.where(inside, offsets, 0.0)
    kernel = jnp.where(
        inside, jnp.exp(-math.pi * safe_off * safe_off / (8.0 * spread * spread)), 0.0
    )
    norm_total = jnp.sqrt(jnp.sum(kernel * kernel, axis=axis, keepdims=True))
    return (kernel / norm_total).astype(jnp.bfloat16)


def offsets_of(shape, in_axis, margin):
    return (
        lax.broadcasted_iota(jnp.int32, shape, in_axis)
        - margin
        - lax.broadcasted_iota(jnp.int32, shape, 1 - in_axis)
    ).astype(jnp.float32)


def filter_kernel(
    n_wall,
    n_span,
    noise_ref,
    widths_ref,
    fluct_ref,
    total_ref,
    stage,
    pad,
    wide,
    wall_band,
    span_band,
    last,
    moments,
    gather,
    noise_sem,
    wall_send,
    wall_recv,
    span_send,
    span_recv,
    sum_send,
    sum_recv,
):
    chunks, n_comp, chunk, n_cols, width = pad.shape
    n_rows = widths_ref.shape[1]
    margin = (width - n_rows) // 2
    span_margin = (wide.shape[3] - n_cols) // 2
    wall = lax.axis_index("wall")
    span = lax.axis_index("span")
    after = lax.rem(span + 1, n_span)
    before = lax.rem(span + n_span - 1, n_span)
    low = wall > 0
    high = wall < n_wall - 1

    def noise_copy(i):
        return pltpu.make_async_copy(
            noise_ref.at[:, pl.ds(i * chunk, chunk)], stage.at[i], noise_sem.at[i]
        )

    def to_lower(i):
        return pltpu.make_async_remote_copy(
            src_ref=pad.at[i, :, :, :, pl.ds(margin, margin)],
            dst_ref=pad.at[i, :, :, :, pl.ds(margin + n_rows, margin)],
            send_sem=wall_send.at[0, i],
            recv_sem=wall_recv.at[0, i],
            device_id={"wall": wall - 1},
            device_id_type=MESH,
        )

    def to_upper(i):
        return pltpu.make_async_remote_copy(
            src_ref=pad.at[i, :, :, :, pl.ds(n_rows, margin)],
            dst_ref=pad.at[i, :, :, :, pl.ds(0, margin)],
            send_sem=wall_send.at[1, i],
            recv_sem=wall_recv.at[1, i],
            device_id={"wall": wall + 1},
            device_id_type=MESH,
        )

    def to_before(i):
        return pltpu.make_async_remote_copy(
            src_ref=wide.at[i, :, :, pl.ds(span_margin, span_margin)],
            dst_ref=wide.at[i, :, :, pl.ds(span_margin + n_cols, span_margin)],
            send_sem=span_send.at[0, i],
            recv_sem=span_recv.at[0, i],
            device_id={"span": before},
            device_id_type=MESH,
        )

    def to_after(i):
        return pltpu.make_async_remote_copy(
            src_ref=wide.at[i, :, :, pl.ds(n_cols, span_margin)],
            dst_ref=wide.at[i, :, :, pl.ds(0, span_margin)],
            send_sem=span_send.at[1, i],
            recv_sem=span_recv.at[1, i],
            device_id={"span": after},
            device_id_type=MESH,
        )

    def sum_copy(k):
        return pltpu.make_async_remote_copy(
            src_ref=gather.at[span],
            dst_ref=gather.at[span],
            send_sem=sum_send.at[k],
            recv_sem=sum_recv.at[span],
            device_id={"span": lax.rem(span + k, n_span)},
            device_id_type=MESH,
        )

    barrier = pltpu.get_barrier_semaphore()
    for k in range(1, n_span):
        pl.semaphore_signal(
            barrier, inc=1, device_id={"span": lax.rem(span + k, n_span)}, device_id_type=MESH
        )

    @pl.when(low)
    def _():
        pl.semaphore_signal(barrier, inc=1, device_id={"wall": wall - 1}, device_id_type=MESH)

    @pl.when(high)
    def _():
        pl.semaphore_signal(barrier, inc=1, device_id={"wall": wall + 1}, device_id_type=MESH)

    @pl.loop(0, chunks)
    def _(i):
        noise_copy(i).start()

    def convert(i):
        noise_copy(i).wait()
        for c in range(n_comp):
            for s in range(chunk):
                pad[i, c, s, :, margin : margin + n_rows] = to_field(stage[i, c, s])

    def send_walls(i):
        @pl.when(low)
        def _():
            to_lower(i).start()

        @pl.when(high)
        def _():
            to_upper(i).start()

    convert(0)
    pl.semaphore_wait(
        barrier, n_span - 1 + low.astype(jnp.int32) + high.astype(jnp.int32)
    )
    send_walls(0)

    @pl.loop(1, min(AHEAD, chunks))
    def _(i):
        convert(i)
        send_walls(i)

    wall_band[...] = band_taps(
        offsets_of((width, n_rows), 0, margin), widths_ref[...].astype(jnp.float32), 0
    )
    span_band[...] = band_taps(
        offsets_of((n_cols, n_cols + 2 * span_margin), 1, span_margin),
        jnp.full((n_cols, 1), float(SPANW), jnp.float32),
        1,
    )

    @pl.when(jnp.logical_not(low))
    def _():
        @pl.loop(0, chunks)
        def _(i):
            pad[i, :, :, :, 0:margin] = jnp.zeros((n_comp, chunk, n_cols, margin), jnp.bfloat16)

    @pl.when(jnp.logical_not(high))
    def _():
        @pl.loop(0, chunks)
        def _(i):
            pad[i, :, :, :, margin + n_rows : width] = jnp.zeros(
                (n_comp, chunk, n_cols, margin), jnp.bfloat16
            )

    @pl.loop(0, chunks)
    def _(i):
        @pl.when(low)
        def _():
            to_upper(i).wait_recv()

        @pl.when(high)
        def _():
            to_lower(i).wait_recv()

        window = pad[i].reshape(n_comp * chunk * n_cols, width)
        smooth = jnp.dot(window, wall_band[...], preferred_element_type=jnp.float32)
        wide[i, :, :, span_margin : span_margin + n_cols] = smooth.astype(jnp.bfloat16).reshape(
            n_comp, chunk, n_cols, n_rows
        )
        to_before(i).start()
        to_after(i).start()

        @pl.when(i + AHEAD < chunks)
        def _():
            convert(i + AHEAD)
            send_walls(i + AHEAD)

    decay = math.exp(-math.pi / (2.0 * TSCALE))
    fresh = math.sqrt(1.0 - decay * decay)
    last[...] = jnp.zeros_like(last)
    moments[...] = jnp.zeros_like(moments)

    def fold(values):
        return jnp.sum(values.reshape(n_cols // 8, 8, n_rows), axis=0)

    @pl.loop(0, chunks)
    def _(i):
        to_before(i).wait_recv()
        to_after(i).wait_recv()
        for s in range(chunk):
            gain = jnp.where(i * chunk + s == 0, 1.0, fresh).astype(jnp.float32)
            now = []
            for c in range(n_comp):
                spanned = jnp.dot(
                    span_band[...], wide[i, c, s], preferred_element_type=jnp.float32
                )
                value = decay * last[c] + gain * spanned
                last[c] = value
                fluct_ref[c, i * chunk + s] = value
                now.append(value)
            for c in range(n_comp):
                moments[c] += fold(now[c])
            for slot, (one, two) in enumerate(PAIRS):
                moments[n_comp + slot] += fold(now[one] * now[two])

    gather[span] = jnp.sum(moments[...], axis=1)
    for k in range(1, n_span):
        sum_copy(k).start()

    @pl.loop(0, chunks)
    def _(i):
        @pl.when(low)
        def _():
            to_lower(i).wait_send()

        @pl.when(high)
        def _():
            to_upper(i).wait_send()

        to_before(i).wait_send()
        to_after(i).wait_send()

    for k in range(1, n_span):
        source = lax.rem(span + k, n_span)
        pltpu.make_async_remote_copy(
            src_ref=gather.at[span],
            dst_ref=gather.at[source],
            send_sem=sum_send.at[k],
            recv_sem=sum_recv.at[source],
            device_id={"span": source},
            device_id_type=MESH,
        ).wait_recv()
    total = gather[0]
    for k in range(1, n_span):
        total = total + gather[k]
    total_ref[...] = total
    for k in range(1, n_span):
        sum_copy(k).wait_send()


def scale_kernel(cell_count, fluct_ref, total_ref, mean_ref, diag_ref, lower_ref, out_ref, rows):
    @pl.when(pl.program_id(0) == 0)
    def _():
        means = [total_ref[c : c + 1] / cell_count for c in range(3)]
        spread = [
            total_ref[3 + slot : 4 + slot] / cell_count - means[one] * means[two]
            for slot, (one, two) in enumerate(PAIRS)
        ]
        gains = lund_transform(
            spread,
            [diag_ref[c : c + 1] for c in range(3)],
            [lower_ref[c : c + 1] for c in range(3)],
        )
        for slot, row in enumerate(means + list(gains)):
            rows[slot : slot + 1] = row

    row = [rows[slot : slot + 1] for slot in range(9)]
    mean = [mean_ref[c : c + 1] for c in range(3)]
    first = pl.program_id(0) * out_ref.shape[1]
    for s in range(out_ref.shape[1]):
        centred = [fluct_ref[c, first + s] - row[c] for c in range(3)]
        out_ref[0, s] = mean[0] + row[3] * centred[0]
        out_ref[1, s] = mean[1] + row[4] * centred[0] + row[5] * centred[1]
        out_ref[2, s] = mean[2] + row[6] * centred[0] + row[7] * centred[1] + row[8] * centred[2]


def shards(
    noise_bits, filter_widths, target_mean_profile, target_factor_diagonal, target_factor_lower
):
    n_comp, n_samples, n_cols, n_rows = noise_bits.shape
    n_wall, n_span = lax.axis_size("wall"), lax.axis_size("span")
    margin = 2 * WMAX
    span_margin = 2 * SPANW
    chunks = n_samples // CHUNK
    n_sums = n_comp + len(PAIRS)
    vmem = pl.BlockSpec(memory_space=pltpu.VMEM)
    fluct, total = pl.pallas_call(
        functools.partial(filter_kernel, n_wall, n_span),
        out_shape=[
            pltpu.VMEM(noise_bits.shape, jnp.float32),
            pltpu.VMEM((n_sums, n_rows), jnp.float32),
        ],
        in_specs=[pl.BlockSpec(memory_space=pl.ANY), vmem],
        out_specs=[vmem, vmem],
        scratch_shapes=[
            pltpu.VMEM((chunks, n_comp, CHUNK, n_cols, n_rows), jnp.int32),
            pltpu.VMEM((chunks, n_comp, CHUNK, n_cols, n_rows + 2 * margin), jnp.bfloat16),
            pltpu.VMEM((chunks, n_comp, CHUNK, n_cols + 2 * span_margin, n_rows), jnp.bfloat16),
            pltpu.VMEM((n_rows + 2 * margin, n_rows), jnp.bfloat16),
            pltpu.VMEM((n_cols, n_cols + 2 * span_margin), jnp.bfloat16),
            pltpu.VMEM((n_comp, n_cols, n_rows), jnp.float32),
            pltpu.VMEM((n_sums, 8, n_rows), jnp.float32),
            pltpu.VMEM((n_span, n_sums, n_rows), jnp.float32),
            pltpu.SemaphoreType.DMA((chunks,)),
            pltpu.SemaphoreType.DMA((2, chunks)),
            pltpu.SemaphoreType.DMA((2, chunks)),
            pltpu.SemaphoreType.DMA((2, chunks)),
            pltpu.SemaphoreType.DMA((2, chunks)),
            pltpu.SemaphoreType.DMA((n_span,)),
            pltpu.SemaphoreType.DMA((n_span,)),
        ],
        compiler_params=pltpu.CompilerParams(
            collective_id=0, has_side_effects=True, vmem_limit_bytes=54 * 1024 * 1024
        ),
        name="filters",
    )(noise_bits, filter_widths.reshape(1, n_rows))
    block = (n_comp, BLOCK, n_cols, n_rows)
    return pl.pallas_call(
        functools.partial(scale_kernel, float(n_samples * n_cols * n_span)),
        out_shape=jax.ShapeDtypeStruct(noise_bits.shape, jnp.float32),
        grid=(n_samples // BLOCK,),
        in_specs=[vmem, vmem, vmem, vmem, vmem],
        out_specs=pl.BlockSpec(block, lambda i: (0, i, 0, 0)),
        scratch_shapes=[pltpu.VMEM((9, n_rows), jnp.float32)],
        compiler_params=pltpu.CompilerParams(vmem_limit_bytes=16 * 1024 * 1024),
        name="rescale",
    )(fluct, total, target_mean_profile, target_factor_diagonal, target_factor_lower)


def solution(mesh):
    placed = (
        P(None, None, "span", "wall"),
        P("wall"),
        P(None, "wall"),
        P(None, "wall"),
        P(None, "wall"),
    )
    return jax.shard_map(
        shards, mesh=mesh, in_specs=placed, out_specs=P(None, None, "span", "wall"), check_vma=False
    )
```

```python
import functools
import math

import jax
import jax.numpy as jnp
from jax import lax
from jax.experimental import pallas as pl
from jax.experimental.pallas import tpu as pltpu
from jax.sharding import PartitionSpec as P

WMAX = 64
SPANW = 32
TSCALE = 8


PAIRS = ((0, 0), (1, 0), (1, 1), (2, 0), (2, 1), (2, 2))
SPREAD_FLOOR = 0.25
INV_RANGE = 1.0 / 1073741824.0


def to_field(noise_bits):
    scaled = (noise_bits.astype(jnp.float32) + 0.5) * INV_RANGE - 0.5
    return (math.sqrt(12.0) * scaled).astype(jnp.bfloat16)


def lund_transform(sample_covariance, target_factor_diagonal, target_factor_lower):
    cov_00 = sample_covariance[0] + SPREAD_FLOOR
    cov_10 = sample_covariance[1]
    cov_11 = sample_covariance[2] + SPREAD_FLOOR
    cov_20 = sample_covariance[3]
    cov_21 = sample_covariance[4]
    cov_22 = sample_covariance[5] + SPREAD_FLOOR
    chol_00 = jnp.sqrt(cov_00)
    chol_10 = cov_10 / chol_00
    chol_20 = cov_20 / chol_00
    chol_11 = jnp.sqrt(cov_11 - chol_10 * chol_10)
    chol_21 = (cov_21 - chol_20 * chol_10) / chol_11
    chol_22 = jnp.sqrt(cov_22 - chol_20 * chol_20 - chol_21 * chol_21)
    inv_00 = 1.0 / chol_00
    inv_11 = 1.0 / chol_11
    inv_22 = 1.0 / chol_22
    inv_10 = -chol_10 * inv_00 * inv_11
    inv_21 = -chol_21 * inv_11 * inv_22
    inv_20 = -(chol_20 * inv_00 + chol_21 * inv_10) * inv_22
    gain_00 = target_factor_diagonal[0] * inv_00
    gain_10 = target_factor_lower[0] * inv_00 + target_factor_diagonal[1] * inv_10
    gain_11 = target_factor_diagonal[1] * inv_11
    gain_20 = (
        target_factor_lower[1] * inv_00
        + target_factor_lower[2] * inv_10
        + target_factor_diagonal[2] * inv_20
    )
    gain_21 = target_factor_lower[2] * inv_11 + target_factor_diagonal[2] * inv_21
    gain_22 = target_factor_diagonal[2] * inv_22
    return gain_00, gain_10, gain_11, gain_20, gain_21, gain_22


CHUNK = 1
EARLY = 2
AHEAD = 6
BLOCK = 2
MESH = pl.DeviceIdType.MESH


def band_taps(offsets, spread, axis):
    inside = jnp.abs(offsets) <= 2.0 * spread
    safe_off = jnp.where(inside, offsets, 0.0)
    kernel = jnp.where(
        inside, jnp.exp(-math.pi * safe_off * safe_off / (8.0 * spread * spread)), 0.0
    )
    norm_total = jnp.sqrt(jnp.sum(kernel * kernel, axis=axis, keepdims=True))
    return (kernel / norm_total).astype(jnp.bfloat16)


def offsets_of(shape, in_axis, margin):
    return (
        lax.broadcasted_iota(jnp.int32, shape, in_axis)
        - margin
        - lax.broadcasted_iota(jnp.int32, shape, 1 - in_axis)
    ).astype(jnp.float32)


def filter_kernel(
    n_wall,
    n_span,
    noise_ref,
    widths_ref,
    fluct_ref,
    total_ref,
    widths_vmem,
    stage,
    pad,
    wide,
    wall_band,
    span_band,
    last,
    moments,
    gather,
    widths_sem,
    noise_sem,
    wall_send,
    wall_recv,
    span_send,
    span_recv,
    sum_send,
    sum_recv,
):
    chunks, n_comp, chunk, n_cols, width = pad.shape
    n_rows = widths_ref.shape[1]
    margin = (width - n_rows) // 2
    span_margin = (wide.shape[3] - n_cols) // 2
    wall = lax.axis_index("wall")
    span = lax.axis_index("span")
    after = lax.rem(span + 1, n_span)
    before = lax.rem(span + n_span - 1, n_span)
    low = wall > 0
    high = wall < n_wall - 1

    def noise_copy(i):
        return pltpu.make_async_copy(
            noise_ref.at[:, pl.ds(i * chunk, chunk)], stage.at[i], noise_sem.at[i]
        )

    def to_lower(i):
        return pltpu.make_async_remote_copy(
            src_ref=pad.at[i, :, :, :, pl.ds(margin, margin)],
            dst_ref=pad.at[i, :, :, :, pl.ds(margin + n_rows, margin)],
            send_sem=wall_send.at[0, i],
            recv_sem=wall_recv.at[0, i],
            device_id={"wall": wall - 1},
            device_id_type=MESH,
        )

    def to_upper(i):
        return pltpu.make_async_remote_copy(
            src_ref=pad.at[i, :, :, :, pl.ds(n_rows, margin)],
            dst_ref=pad.at[i, :, :, :, pl.ds(0, margin)],
            send_sem=wall_send.at[1, i],
            recv_sem=wall_recv.at[1, i],
            device_id={"wall": wall + 1},
            device_id_type=MESH,
        )

    def to_before(i):
        return pltpu.make_async_remote_copy(
            src_ref=wide.at[i, :, :, pl.ds(span_margin, span_margin)],
            dst_ref=wide.at[i, :, :, pl.ds(span_margin + n_cols, span_margin)],
            send_sem=span_send.at[0, i],
            recv_sem=span_recv.at[0, i],
            device_id={"span": before},
            device_id_type=MESH,
        )

    def to_after(i):
        return pltpu.make_async_remote_copy(
            src_ref=wide.at[i, :, :, pl.ds(n_cols, span_margin)],
            dst_ref=wide.at[i, :, :, pl.ds(0, span_margin)],
            send_sem=span_send.at[1, i],
            recv_sem=span_recv.at[1, i],
            device_id={"span": after},
            device_id_type=MESH,
        )

    def sum_copy(k):
        return pltpu.make_async_remote_copy(
            src_ref=gather.at[span],
            dst_ref=gather.at[span],
            send_sem=sum_send.at[k],
            recv_sem=sum_recv.at[span],
            device_id={"span": lax.rem(span + k, n_span)},
            device_id_type=MESH,
        )

    early = min(EARLY, chunks - 1)
    ready = min(early + AHEAD, chunks)
    for i in range(early):
        noise_copy(i).start()
    barrier = pltpu.get_barrier_semaphore()
    for k in range(1, n_span):
        pl.semaphore_signal(
            barrier, inc=1, device_id={"span": lax.rem(span + k, n_span)}, device_id_type=MESH
        )

    @pl.when(low)
    def _():
        pl.semaphore_signal(barrier, inc=1, device_id={"wall": wall - 1}, device_id_type=MESH)

    @pl.when(high)
    def _():
        pl.semaphore_signal(barrier, inc=1, device_id={"wall": wall + 1}, device_id_type=MESH)

    widths_copy = pltpu.make_async_copy(widths_ref, widths_vmem, widths_sem)
    for i in range(early, early + 2):
        noise_copy(i).start()
    widths_copy.start()

    def convert(i):
        noise_copy(i).wait()
        for c in range(n_comp):
            for s in range(chunk):
                pad[i, c, s, :, margin : margin + n_rows] = to_field(stage[i, c, s])

    def convert_early(i):
        noise_copy(i).wait()
        for c in range(n_comp):
            for s in range(chunk):
                wide[i, c, s, span_margin : span_margin + n_cols] = to_field(stage[i, c, s])

    def send_walls(i):
        @pl.when(low)
        def _():
            to_lower(i).start()

        @pl.when(high)
        def _():
            to_upper(i).start()

    convert_early(0)
    pl.semaphore_wait(
        barrier, n_span - 1 + low.astype(jnp.int32) + high.astype(jnp.int32)
    )
    to_before(0).start()
    to_after(0).start()
    for i in range(1, early):
        convert_early(i)
        to_before(i).start()
        to_after(i).start()

    @pl.loop(early + 2, chunks)
    def _(i):
        noise_copy(i).start()

    @pl.loop(early, ready)
    def _(i):
        convert(i)
        send_walls(i)

    widths_copy.wait()
    wall_band[...] = band_taps(
        offsets_of((width, n_rows), 0, margin), widths_vmem[...].astype(jnp.float32), 0
    )
    span_band[...] = band_taps(
        offsets_of((n_cols, n_cols + 2 * span_margin), 1, span_margin),
        jnp.full((n_cols, 1), float(SPANW), jnp.float32),
        1,
    )

    @pl.when(jnp.logical_not(low))
    def _():
        @pl.loop(0, chunks)
        def _(i):
            pad[i, :, :, :, 0:margin] = jnp.zeros((n_comp, chunk, n_cols, margin), jnp.bfloat16)

    @pl.when(jnp.logical_not(high))
    def _():
        @pl.loop(0, chunks)
        def _(i):
            pad[i, :, :, :, margin + n_rows : width] = jnp.zeros(
                (n_comp, chunk, n_cols, margin), jnp.bfloat16
            )

    def wait_walls(i):
        @pl.when(low)
        def _():
            to_upper(i).wait_recv()

        @pl.when(high)
        def _():
            to_lower(i).wait_recv()

    def wall_filter(i):
        window = pad[i].reshape(n_comp * chunk * n_cols, width)
        smooth = jnp.dot(window, wall_band[...], preferred_element_type=jnp.float32)
        return smooth.reshape(n_comp, chunk, n_cols, n_rows)

    def span_filter(i, c, s):
        return jnp.dot(span_band[...], wide[i, c, s], preferred_element_type=jnp.float32)

    @pl.loop(early, chunks)
    def _(i):
        wait_walls(i)
        wide[i, :, :, span_margin : span_margin + n_cols] = wall_filter(i).astype(jnp.bfloat16)
        to_before(i).start()
        to_after(i).start()

        @pl.when(i + ready - early < chunks)
        def _():
            convert(i + ready - early)
            send_walls(i + ready - early)

    for i in range(early):
        to_before(i).wait_recv()
        to_after(i).wait_recv()
        for c in range(n_comp):
            for s in range(chunk):
                pad[i, c, s, :, margin : margin + n_rows] = span_filter(i, c, s).astype(
                    jnp.bfloat16
                )
        send_walls(i)

    decay = math.exp(-math.pi / (2.0 * TSCALE))
    fresh = math.sqrt(1.0 - decay * decay)
    last[...] = jnp.zeros_like(last)
    moments[...] = jnp.zeros_like(moments)

    def fold(values):
        return jnp.sum(values.reshape(n_cols // 8, 8, n_rows), axis=0)

    def advance(time, spanned):
        gain = jnp.where(time == 0, 1.0, fresh).astype(jnp.float32)
        now = []
        for c in range(n_comp):
            value = decay * last[c] + gain * spanned(c)
            last[c] = value
            fluct_ref[c, time] = value
            now.append(value)
        for c in range(n_comp):
            moments[c] += fold(now[c])
        for slot, (one, two) in enumerate(PAIRS):
            moments[n_comp + slot] += fold(now[one] * now[two])

    for i in range(early):
        wait_walls(i)
        filtered = wall_filter(i)
        for s in range(chunk):
            advance(i * chunk + s, lambda c: filtered[c, s])

    @pl.loop(early, chunks)
    def _(i):
        to_before(i).wait_recv()
        to_after(i).wait_recv()
        for s in range(chunk):
            advance(i * chunk + s, lambda c: span_filter(i, c, s))

    gather[span] = jnp.sum(moments[...], axis=1)
    for k in range(1, n_span):
        sum_copy(k).start()

    @pl.loop(0, chunks)
    def _(i):
        @pl.when(low)
        def _():
            to_lower(i).wait_send()

        @pl.when(high)
        def _():
            to_upper(i).wait_send()

        to_before(i).wait_send()
        to_after(i).wait_send()

    for k in range(1, n_span):
        source = lax.rem(span + k, n_span)
        pltpu.make_async_remote_copy(
            src_ref=gather.at[span],
            dst_ref=gather.at[source],
            send_sem=sum_send.at[k],
            recv_sem=sum_recv.at[source],
            device_id={"span": source},
            device_id_type=MESH,
        ).wait_recv()
    total = gather[0]
    for k in range(1, n_span):
        total = total + gather[k]
    total_ref[...] = total
    for k in range(1, n_span):
        sum_copy(k).wait_send()


def scale_kernel(
    cell_count, fluct_ref, total_ref, mean_ref, diag_ref, lower_ref, out_ref, scaled, out_sem
):
    n_rows = total_ref.shape[1]
    blocks = scaled.shape[1] // BLOCK
    means = [total_ref[c : c + 1] / cell_count for c in range(3)]
    spread = [
        total_ref[3 + slot : 4 + slot] / cell_count - means[one] * means[two]
        for slot, (one, two) in enumerate(PAIRS)
    ]
    gains = lund_transform(
        spread,
        [diag_ref[c : c + 1] for c in range(3)],
        [lower_ref[c : c + 1] for c in range(3)],
    )
    row = [jnp.broadcast_to(value, (8, n_rows)) for value in means + list(gains)]
    mean = [jnp.broadcast_to(mean_ref[c : c + 1], (8, n_rows)) for c in range(3)]

    def out_copy(i):
        piece = pl.ds(i * BLOCK, BLOCK)
        return pltpu.make_async_copy(scaled.at[:, piece], out_ref.at[:, piece], out_sem.at[i])

    @pl.loop(0, blocks)
    def _(i):
        for s in range(BLOCK):
            time = i * BLOCK + s
            for j in range(0, scaled.shape[2], 8):
                centred = [fluct_ref[c, time, j : j + 8] - row[c] for c in range(3)]
                scaled[0, time, j : j + 8] = mean[0] + row[3] * centred[0]
                scaled[1, time, j : j + 8] = (
                    mean[1] + row[4] * centred[0] + row[5] * centred[1]
                )
                scaled[2, time, j : j + 8] = (
                    mean[2] + row[6] * centred[0] + row[7] * centred[1] + row[8] * centred[2]
                )
        out_copy(i).start()

    @pl.loop(0, blocks)
    def _(i):
        out_copy(i).wait()


def shards(
    noise_bits, filter_widths, target_mean_profile, target_factor_diagonal, target_factor_lower
):
    n_comp, n_samples, n_cols, n_rows = noise_bits.shape
    n_wall, n_span = lax.axis_size("wall"), lax.axis_size("span")
    margin = 2 * WMAX
    span_margin = 2 * SPANW
    chunks = n_samples // CHUNK
    n_sums = n_comp + len(PAIRS)
    vmem = pl.BlockSpec(memory_space=pltpu.VMEM)
    fluct, total = pl.pallas_call(
        functools.partial(filter_kernel, n_wall, n_span),
        out_shape=[
            pltpu.VMEM(noise_bits.shape, jnp.float32),
            pltpu.VMEM((n_sums, n_rows), jnp.float32),
        ],
        in_specs=[pl.BlockSpec(memory_space=pl.ANY)] * 2,
        out_specs=[vmem, vmem],
        scratch_shapes=[
            pltpu.VMEM((1, n_rows), jnp.int32),
            pltpu.VMEM((chunks, n_comp, CHUNK, n_cols, n_rows), jnp.int32),
            pltpu.VMEM((chunks, n_comp, CHUNK, n_cols, n_rows + 2 * margin), jnp.bfloat16),
            pltpu.VMEM((chunks, n_comp, CHUNK, n_cols + 2 * span_margin, n_rows), jnp.bfloat16),
            pltpu.VMEM((n_rows + 2 * margin, n_rows), jnp.bfloat16),
            pltpu.VMEM((n_cols, n_cols + 2 * span_margin), jnp.bfloat16),
            pltpu.VMEM((n_comp, n_cols, n_rows), jnp.float32),
            pltpu.VMEM((n_sums, 8, n_rows), jnp.float32),
            pltpu.VMEM((n_span, n_sums, n_rows), jnp.float32),
            pltpu.SemaphoreType.DMA,
            pltpu.SemaphoreType.DMA((chunks,)),
            pltpu.SemaphoreType.DMA((2, chunks)),
            pltpu.SemaphoreType.DMA((2, chunks)),
            pltpu.SemaphoreType.DMA((2, chunks)),
            pltpu.SemaphoreType.DMA((2, chunks)),
            pltpu.SemaphoreType.DMA((n_span,)),
            pltpu.SemaphoreType.DMA((n_span,)),
        ],
        compiler_params=pltpu.CompilerParams(
            collective_id=0, has_side_effects=True, vmem_limit_bytes=54 * 1024 * 1024
        ),
        name="filters",
    )(noise_bits, filter_widths.reshape(1, n_rows))
    return pl.pallas_call(
        functools.partial(scale_kernel, float(n_samples * n_cols * n_span)),
        out_shape=jax.ShapeDtypeStruct(noise_bits.shape, jnp.float32),
        in_specs=[vmem] * 5,
        out_specs=pl.BlockSpec(memory_space=pl.ANY),
        scratch_shapes=[
            pltpu.VMEM(noise_bits.shape, jnp.float32),
            pltpu.SemaphoreType.DMA((n_samples // BLOCK,)),
        ],
        compiler_params=pltpu.CompilerParams(vmem_limit_bytes=16 * 1024 * 1024),
        name="rescale",
    )(fluct, total, target_mean_profile, target_factor_diagonal, target_factor_lower)


def solution(mesh):
    placed = (
        P(None, None, "span", "wall"),
        P("wall"),
        P(None, "wall"),
        P(None, "wall"),
        P(None, "wall"),
    )
    return jax.shard_map(
        shards, mesh=mesh, in_specs=placed, out_specs=P(None, None, "span", "wall"), check_vma=False
    )
```

```python
import functools
import math

import jax
import jax.numpy as jnp
from jax import lax
from jax.experimental import pallas as pl
from jax.experimental.pallas import tpu as pltpu
from jax.sharding import PartitionSpec as P

WMAX = 64
SPANW = 32
TSCALE = 8


PAIRS = ((0, 0), (1, 0), (1, 1), (2, 0), (2, 1), (2, 2))
SPREAD_FLOOR = 0.25
INV_RANGE = 1.0 / 1073741824.0


def to_field(noise_bits):
    scaled = (noise_bits.astype(jnp.float32) + 0.5) * INV_RANGE - 0.5
    return (math.sqrt(12.0) * scaled).astype(jnp.bfloat16)


def lund_transform(sample_covariance, target_factor_diagonal, target_factor_lower):
    cov_00 = sample_covariance[0] + SPREAD_FLOOR
    cov_10 = sample_covariance[1]
    cov_11 = sample_covariance[2] + SPREAD_FLOOR
    cov_20 = sample_covariance[3]
    cov_21 = sample_covariance[4]
    cov_22 = sample_covariance[5] + SPREAD_FLOOR
    chol_00 = jnp.sqrt(cov_00)
    chol_10 = cov_10 / chol_00
    chol_20 = cov_20 / chol_00
    chol_11 = jnp.sqrt(cov_11 - chol_10 * chol_10)
    chol_21 = (cov_21 - chol_20 * chol_10) / chol_11
    chol_22 = jnp.sqrt(cov_22 - chol_20 * chol_20 - chol_21 * chol_21)
    inv_00 = 1.0 / chol_00
    inv_11 = 1.0 / chol_11
    inv_22 = 1.0 / chol_22
    inv_10 = -chol_10 * inv_00 * inv_11
    inv_21 = -chol_21 * inv_11 * inv_22
    inv_20 = -(chol_20 * inv_00 + chol_21 * inv_10) * inv_22
    gain_00 = target_factor_diagonal[0] * inv_00
    gain_10 = target_factor_lower[0] * inv_00 + target_factor_diagonal[1] * inv_10
    gain_11 = target_factor_diagonal[1] * inv_11
    gain_20 = (
        target_factor_lower[1] * inv_00
        + target_factor_lower[2] * inv_10
        + target_factor_diagonal[2] * inv_20
    )
    gain_21 = target_factor_lower[2] * inv_11 + target_factor_diagonal[2] * inv_21
    gain_22 = target_factor_diagonal[2] * inv_22
    return gain_00, gain_10, gain_11, gain_20, gain_21, gain_22


CHUNK = 2
EARLY = 2
AHEAD = 3
BLOCK = 2
MESH = pl.DeviceIdType.MESH


def band_taps(offsets, spread, axis):
    inside = jnp.abs(offsets) <= 2.0 * spread
    safe_off = jnp.where(inside, offsets, 0.0)
    kernel = jnp.where(
        inside, jnp.exp(-math.pi * safe_off * safe_off / (8.0 * spread * spread)), 0.0
    )
    norm_total = jnp.sqrt(jnp.sum(kernel * kernel, axis=axis, keepdims=True))
    return (kernel / norm_total).astype(jnp.bfloat16)


def offsets_of(shape, in_axis, margin):
    return (
        lax.broadcasted_iota(jnp.int32, shape, in_axis)
        - margin
        - lax.broadcasted_iota(jnp.int32, shape, 1 - in_axis)
    ).astype(jnp.float32)


def filter_kernel(
    n_wall,
    n_span,
    noise_ref,
    widths_ref,
    fluct_ref,
    total_ref,
    widths_vmem,
    stage,
    pad,
    wide,
    wall_band,
    span_band,
    last,
    moments,
    gather,
    widths_sem,
    noise_sem,
    wall_send,
    wall_recv,
    span_send,
    span_recv,
    sum_send,
    sum_recv,
):
    chunks, n_comp, chunk, n_cols, width = pad.shape
    n_rows = widths_ref.shape[1]
    margin = (width - n_rows) // 2
    span_margin = (wide.shape[3] - n_cols) // 2
    wall = lax.axis_index("wall")
    span = lax.axis_index("span")
    after = lax.rem(span + 1, n_span)
    before = lax.rem(span + n_span - 1, n_span)
    low = wall > 0
    high = wall < n_wall - 1

    def noise_copy(i):
        return pltpu.make_async_copy(
            noise_ref.at[:, pl.ds(i * chunk, chunk)], stage.at[i], noise_sem.at[i]
        )

    def to_lower(i):
        return pltpu.make_async_remote_copy(
            src_ref=pad.at[i, :, :, :, pl.ds(margin, margin)],
            dst_ref=pad.at[i, :, :, :, pl.ds(margin + n_rows, margin)],
            send_sem=wall_send.at[0, i],
            recv_sem=wall_recv.at[0, i],
            device_id={"wall": wall - 1},
            device_id_type=MESH,
        )

    def to_upper(i):
        return pltpu.make_async_remote_copy(
            src_ref=pad.at[i, :, :, :, pl.ds(n_rows, margin)],
            dst_ref=pad.at[i, :, :, :, pl.ds(0, margin)],
            send_sem=wall_send.at[1, i],
            recv_sem=wall_recv.at[1, i],
            device_id={"wall": wall + 1},
            device_id_type=MESH,
        )

    def to_before(i):
        return pltpu.make_async_remote_copy(
            src_ref=wide.at[i, :, :, pl.ds(span_margin, span_margin)],
            dst_ref=wide.at[i, :, :, pl.ds(span_margin + n_cols, span_margin)],
            send_sem=span_send.at[0, i],
            recv_sem=span_recv.at[0, i],
            device_id={"span": before},
            device_id_type=MESH,
        )

    def to_after(i):
        return pltpu.make_async_remote_copy(
            src_ref=wide.at[i, :, :, pl.ds(n_cols, span_margin)],
            dst_ref=wide.at[i, :, :, pl.ds(0, span_margin)],
            send_sem=span_send.at[1, i],
            recv_sem=span_recv.at[1, i],
            device_id={"span": after},
            device_id_type=MESH,
        )

    def sum_copy(k):
        return pltpu.make_async_remote_copy(
            src_ref=gather.at[span],
            dst_ref=gather.at[span],
            send_sem=sum_send.at[k],
            recv_sem=sum_recv.at[span],
            device_id={"span": lax.rem(span + k, n_span)},
            device_id_type=MESH,
        )

    early = min(EARLY, chunks - 1)
    ready = min(early + AHEAD, chunks)
    for i in range(early):
        noise_copy(i).start()
    barrier = pltpu.get_barrier_semaphore()
    for k in range(1, n_span):
        pl.semaphore_signal(
            barrier, inc=1, device_id={"span": lax.rem(span + k, n_span)}, device_id_type=MESH
        )

    @pl.when(low)
    def _():
        pl.semaphore_signal(barrier, inc=1, device_id={"wall": wall - 1}, device_id_type=MESH)

    @pl.when(high)
    def _():
        pl.semaphore_signal(barrier, inc=1, device_id={"wall": wall + 1}, device_id_type=MESH)

    widths_copy = pltpu.make_async_copy(widths_ref, widths_vmem, widths_sem)
    for i in range(early, early + 2):
        noise_copy(i).start()
    widths_copy.start()

    def convert(i):
        noise_copy(i).wait()
        for c in range(n_comp):
            for s in range(chunk):
                pad[i, c, s, :, margin : margin + n_rows] = to_field(stage[i, c, s])

    def convert_early(i):
        noise_copy(i).wait()
        for c in range(n_comp):
            for s in range(chunk):
                wide[i, c, s, span_margin : span_margin + n_cols] = to_field(stage[i, c, s])

    def send_walls(i):
        @pl.when(low)
        def _():
            to_lower(i).start()

        @pl.when(high)
        def _():
            to_upper(i).start()

    convert_early(0)
    pl.semaphore_wait(
        barrier, n_span - 1 + low.astype(jnp.int32) + high.astype(jnp.int32)
    )
    to_before(0).start()
    to_after(0).start()
    for i in range(1, early):
        convert_early(i)
        to_before(i).start()
        to_after(i).start()

    @pl.loop(early + 2, chunks)
    def _(i):
        noise_copy(i).start()

    @pl.loop(early, ready)
    def _(i):
        convert(i)
        send_walls(i)

    widths_copy.wait()
    wall_band[...] = band_taps(
        offsets_of((width, n_rows), 0, margin), widths_vmem[...].astype(jnp.float32), 0
    )
    span_band[...] = band_taps(
        offsets_of((n_cols, n_cols + 2 * span_margin), 1, span_margin),
        jnp.full((n_cols, 1), float(SPANW), jnp.float32),
        1,
    )

    @pl.when(jnp.logical_not(low))
    def _():
        @pl.loop(0, chunks)
        def _(i):
            pad[i, :, :, :, 0:margin] = jnp.zeros((n_comp, chunk, n_cols, margin), jnp.bfloat16)

    @pl.when(jnp.logical_not(high))
    def _():
        @pl.loop(0, chunks)
        def _(i):
            pad[i, :, :, :, margin + n_rows : width] = jnp.zeros(
                (n_comp, chunk, n_cols, margin), jnp.bfloat16
            )

    def wait_walls(i):
        @pl.when(low)
        def _():
            to_upper(i).wait_recv()

        @pl.when(high)
        def _():
            to_lower(i).wait_recv()

    def wall_filter(i):
        window = pad[i].reshape(n_comp * chunk * n_cols, width)
        smooth = jnp.dot(window, wall_band[...], preferred_element_type=jnp.float32)
        return smooth.reshape(n_comp, chunk, n_cols, n_rows)

    def span_filter(i, c, s):
        return jnp.dot(span_band[...], wide[i, c, s], preferred_element_type=jnp.float32)

    @pl.loop(early, chunks)
    def _(i):
        wait_walls(i)
        wide[i, :, :, span_margin : span_margin + n_cols] = wall_filter(i).astype(jnp.bfloat16)
        to_before(i).start()
        to_after(i).start()

        @pl.when(i + ready - early < chunks)
        def _():
            convert(i + ready - early)
            send_walls(i + ready - early)

    for i in range(early):
        to_before(i).wait_recv()
        to_after(i).wait_recv()
        for c in range(n_comp):
            for s in range(chunk):
                pad[i, c, s, :, margin : margin + n_rows] = span_filter(i, c, s).astype(
                    jnp.bfloat16
                )
        send_walls(i)

    decay = math.exp(-math.pi / (2.0 * TSCALE))
    fresh = math.sqrt(1.0 - decay * decay)
    last[...] = jnp.zeros_like(last)
    moments[...] = jnp.zeros_like(moments)

    def fold(values):
        return jnp.sum(values.reshape(n_cols // 8, 8, n_rows), axis=0)

    def advance(time, spanned):
        gain = jnp.where(time == 0, 1.0, fresh).astype(jnp.float32)
        now = []
        for c in range(n_comp):
            value = decay * last[c] + gain * spanned(c)
            last[c] = value
            fluct_ref[c, time] = value
            now.append(value)
        for c in range(n_comp):
            moments[c] += fold(now[c])
        for slot, (one, two) in enumerate(PAIRS):
            moments[n_comp + slot] += fold(now[one] * now[two])

    for i in range(early):
        wait_walls(i)
        filtered = wall_filter(i)
        for s in range(chunk):
            advance(i * chunk + s, lambda c: filtered[c, s])

    @pl.loop(early, chunks)
    def _(i):
        to_before(i).wait_recv()
        to_after(i).wait_recv()
        for s in range(chunk):
            advance(i * chunk + s, lambda c: span_filter(i, c, s))

    sums = jnp.sum(moments[...], axis=1)
    for slot in range(sums.shape[0]):
        gather[span, :, slot * n_rows : (slot + 1) * n_rows] = sums[slot : slot + 1]
    for k in range(1, n_span):
        sum_copy(k).start()

    @pl.loop(0, chunks)
    def _(i):
        @pl.when(low)
        def _():
            to_lower(i).wait_send()

        @pl.when(high)
        def _():
            to_upper(i).wait_send()

        to_before(i).wait_send()
        to_after(i).wait_send()

    for k in range(1, n_span):
        source = lax.rem(span + k, n_span)
        pltpu.make_async_remote_copy(
            src_ref=gather.at[span],
            dst_ref=gather.at[source],
            send_sem=sum_send.at[k],
            recv_sem=sum_recv.at[source],
            device_id={"span": source},
            device_id_type=MESH,
        ).wait_recv()
    total = gather[0]
    for k in range(1, n_span):
        total = total + gather[k]
    for slot in range(moments.shape[0]):
        total_ref[slot : slot + 1] = total[:, slot * n_rows : (slot + 1) * n_rows]
    for k in range(1, n_span):
        sum_copy(k).wait_send()


def scale_kernel(
    cell_count, fluct_ref, total_ref, mean_ref, diag_ref, lower_ref, out_ref, scaled, out_sem
):
    n_rows = total_ref.shape[1]
    blocks = scaled.shape[1] // BLOCK
    means = [total_ref[c : c + 1] / cell_count for c in range(3)]
    spread = [
        total_ref[3 + slot : 4 + slot] / cell_count - means[one] * means[two]
        for slot, (one, two) in enumerate(PAIRS)
    ]
    gains = lund_transform(
        spread,
        [diag_ref[c : c + 1] for c in range(3)],
        [lower_ref[c : c + 1] for c in range(3)],
    )
    row = [jnp.broadcast_to(value, (8, n_rows)) for value in means + list(gains)]
    mean = [jnp.broadcast_to(mean_ref[c : c + 1], (8, n_rows)) for c in range(3)]

    def out_copy(i):
        piece = pl.ds(i * BLOCK, BLOCK)
        return pltpu.make_async_copy(scaled.at[:, piece], out_ref.at[:, piece], out_sem.at[i])

    @pl.loop(0, blocks)
    def _(i):
        for s in range(BLOCK):
            time = i * BLOCK + s
            for j in range(0, scaled.shape[2], 8):
                centred = [fluct_ref[c, time, j : j + 8] - row[c] for c in range(3)]
                scaled[0, time, j : j + 8] = mean[0] + row[3] * centred[0]
                scaled[1, time, j : j + 8] = (
                    mean[1] + row[4] * centred[0] + row[5] * centred[1]
                )
                scaled[2, time, j : j + 8] = (
                    mean[2] + row[6] * centred[0] + row[7] * centred[1] + row[8] * centred[2]
                )
        out_copy(i).start()

    @pl.loop(0, blocks)
    def _(i):
        out_copy(i).wait()


def shards(
    noise_bits, filter_widths, target_mean_profile, target_factor_diagonal, target_factor_lower
):
    n_comp, n_samples, n_cols, n_rows = noise_bits.shape
    n_wall, n_span = lax.axis_size("wall"), lax.axis_size("span")
    margin = 2 * WMAX
    span_margin = 2 * SPANW
    chunks = n_samples // CHUNK
    n_sums = n_comp + len(PAIRS)
    vmem = pl.BlockSpec(memory_space=pltpu.VMEM)
    fluct, total = pl.pallas_call(
        functools.partial(filter_kernel, n_wall, n_span),
        out_shape=[
            pltpu.VMEM(noise_bits.shape, jnp.float32),
            pltpu.VMEM((n_sums, n_rows), jnp.float32),
        ],
        in_specs=[pl.BlockSpec(memory_space=pl.ANY)] * 2,
        out_specs=[vmem, vmem],
        scratch_shapes=[
            pltpu.VMEM((1, n_rows), jnp.int32),
            pltpu.VMEM((chunks, n_comp, CHUNK, n_cols, n_rows), jnp.int32),
            pltpu.VMEM((chunks, n_comp, CHUNK, n_cols, n_rows + 2 * margin), jnp.bfloat16),
            pltpu.VMEM((chunks, n_comp, CHUNK, n_cols + 2 * span_margin, n_rows), jnp.bfloat16),
            pltpu.VMEM((n_rows + 2 * margin, n_rows), jnp.bfloat16),
            pltpu.VMEM((n_cols, n_cols + 2 * span_margin), jnp.bfloat16),
            pltpu.VMEM((n_comp, n_cols, n_rows), jnp.float32),
            pltpu.VMEM((n_sums, 8, n_rows), jnp.float32),
            pltpu.VMEM((n_span, 1, n_sums * n_rows), jnp.float32),
            pltpu.SemaphoreType.DMA,
            pltpu.SemaphoreType.DMA((chunks,)),
            pltpu.SemaphoreType.DMA((2, chunks)),
            pltpu.SemaphoreType.DMA((2, chunks)),
            pltpu.SemaphoreType.DMA((2, chunks)),
            pltpu.SemaphoreType.DMA((2, chunks)),
            pltpu.SemaphoreType.DMA((n_span,)),
            pltpu.SemaphoreType.DMA((n_span,)),
        ],
        compiler_params=pltpu.CompilerParams(
            collective_id=0, has_side_effects=True, vmem_limit_bytes=54 * 1024 * 1024
        ),
        name="filters",
    )(noise_bits, filter_widths.reshape(1, n_rows))
    return pl.pallas_call(
        functools.partial(scale_kernel, float(n_samples * n_cols * n_span)),
        out_shape=jax.ShapeDtypeStruct(noise_bits.shape, jnp.float32),
        in_specs=[vmem] * 5,
        out_specs=pl.BlockSpec(memory_space=pl.ANY),
        scratch_shapes=[
            pltpu.VMEM(noise_bits.shape, jnp.float32),
            pltpu.SemaphoreType.DMA((n_samples // BLOCK,)),
        ],
        compiler_params=pltpu.CompilerParams(vmem_limit_bytes=16 * 1024 * 1024),
        name="rescale",
    )(fluct, total, target_mean_profile, target_factor_diagonal, target_factor_lower)


def solution(mesh):
    placed = (
        P(None, None, "span", "wall"),
        P("wall"),
        P(None, "wall"),
        P(None, "wall"),
        P(None, "wall"),
    )
    return jax.shard_map(
        shards, mesh=mesh, in_specs=placed, out_specs=P(None, None, "span", "wall"), check_vma=False
    )
```
